32 devices in a mesh: seq: 4 (over y, x), wshard: 8 (over z, core).
Axes of the slice: x: 2, y: 2, z: 4, core: 2. Of those that a mesh axis runs over, the one named last changes fastest.
Arguments:
- layer_input: bfloat16 [8, 1024, 1536], P('wshard', 'seq'), may hold values from -6 to 6
- lengths: int32 [8], P('wshard'), may hold values from 256 to 1024, as said below
- norm_attn: float32 [1536], replicated, may hold values from 0.1 to 1.9
- w_query: bfloat16 [1536, 1536], P('wshard'), may hold values from -0.15625 to 0.15625
- w_key: bfloat16 [1536, 1536], P('wshard'), may hold values from -0.15625 to 0.15625
- w_value: bfloat16 [1536, 1536], P('wshard'), may hold values from -0.15625 to 0.15625
- w_ogate: bfloat16 [1536, 1536], P('wshard'), may hold values from -0.15625 to 0.15625
- w_forget: bfloat16 [1536, 24], P('wshard'), may hold values from -0.15625 to 0.15625
- forget_bias: float32 [24], replicated, may hold values from 3.5 to 8
- w_out: bfloat16 [1536, 1536], P('wshard'), may hold values from -1 to 1
- norm_ffn: float32 [1536], replicated, may hold values from 0.1 to 1.9
- w_gate: bfloat16 [1536, 4096], P('wshard'), may hold values from -0.15625 to 0.15625
- w_up: bfloat16 [1536, 4096], P('wshard'), may hold values from -0.15625 to 0.15625
- w_down: bfloat16 [4096, 1536], P('wshard'), may hold values from -0.09375 to 0.09375
- output_grad: bfloat16 [8, 1024, 1536], P('wshard', 'seq'), may hold values from -6 to 6
Outputs:
- layer_output: bfloat16 [8, 1024, 1536], P('wshard', 'seq')
- grad_input: float32 [8, 1024, 1536], P('wshard', 'seq')
- grad_norm_attn: float32 [1536], replicated
- grad_w_query: float32 [1536, 1536], P('wshard')
- grad_w_key: float32 [1536, 1536], P('wshard')
- grad_w_value: float32 [1536, 1536], P('wshard')
- grad_w_ogate: float32 [1536, 1536], P('wshard')
- grad_w_forget: float32 [1536, 24], P('wshard')
- grad_forget_bias: float32 [24], replicated
- grad_w_out: float32 [1536, 1536], P('wshard')
- grad_norm_ffn: float32 [1536], replicated
- grad_w_gate: float32 [1536, 4096], P('wshard')
- grad_w_up: float32 [1536, 4096], P('wshard')
- grad_w_down: float32 [4096, 1536], P('wshard')
The draws below stay inside these ranges and needn't reach their ends.
Inputs may be any that keep to these rules, and one draw needn't show every extreme that they name: Each sequence has 1024 slots of which the first lengths[s] are valid; in every draw one sequence is full and one has exactly 256 valid slots.
All inputs are finite; a program needn't handle non-finite values.
Results may differ from the reference program's by a relative error of at most 0.014.
Values may be sent and summed in bfloat16 or wider, within the bound.
A program may use at most 320 MiB of HBM per device.

```python
import jax
import jax.numpy as jnp
from jax import lax

D = 1536
H = 24
FF = 4096
SEQS = 8
SLOTS = 1024


def draw_lengths(key, part):
    lowest = SLOTS // 4
    drawn = jax.random.randint(jax.random.fold_in(key, 11), (SEQS,), lowest, SLOTS + 1, dtype=jnp.int32)
    order = jax.random.permutation(jax.random.fold_in(key, 12), SEQS)
    drawn = drawn.at[order[0]].set(SLOTS)
    drawn = drawn.at[order[1]].set(lowest)
    return drawn.astype(jnp.int32)


def levels(rng, shape, shards, low, high):
    def one(dim, parts):
        steps = jax.random.uniform(jax.random.fold_in(jax.random.fold_in(rng, 6), dim), (parts,), jnp.float32, low / len(shards), high / len(shards))
        return jnp.repeat(jnp.exp(steps), shape[dim] // parts).reshape((-1,) + (1,) * (len(shape) - dim - 1))

    loudness = one(*shards[0])
    for cut in shards[1:]:
        loudness = loudness * one(*cut)
    return loudness


def centred(own_key, extent, scale, most, cuts=(), kind=jnp.bfloat16):
    array = scale * jax.random.normal(own_key, extent, jnp.float32)
    if cuts:
        array = array * levels(own_key, extent, cuts, -0.22, 0.18)
    return jnp.clip(array, -most, most).astype(kind)


def setup_inputs(seed: int = 0) -> dict:
    key_list = jax.random.split(jax.random.key(seed), 16)
    layer_input = centred(key_list[0], (SEQS, SLOTS, D), 1.0, 6.0, ((0, 8), (1, 4)))
    lengths = draw_lengths(jax.random.fold_in(key_list[15], 71), 0)
    norm_attn = jnp.clip(1.0 + 0.18 * jax.random.normal(key_list[2], (D,), jnp.float32), 0.1, 1.9)
    w_query = centred(key_list[3], (D, D), D ** -0.5, 0.15625, ((0, 8),))
    w_key = centred(key_list[4], (D, D), D ** -0.5, 0.15625, ((0, 8),))
    w_value = centred(key_list[5], (D, D), D ** -0.5, 0.15625, ((0, 8),))
    w_ogate = centred(key_list[6], (D, D), D ** -0.5, 0.15625, ((0, 8),))
    w_forget = centred(key_list[7], (D, H), D ** -0.5, 0.15625, ((0, 8),))
    forget_bias = jnp.clip(jax.random.uniform(key_list[8], (H,), jnp.float32, 3.5, 8.0), 3.5, 8.0)
    w_out = centred(key_list[9], (D, D), 32 ** -0.5, 1.0, ((0, 8),))
    norm_ffn = jnp.clip(1.0 + 0.18 * jax.random.normal(key_list[10], (D,), jnp.float32), 0.1, 1.9)
    w_gate = centred(key_list[11], (D, FF), D ** -0.5, 0.15625, ((0, 8),))
    w_up = centred(key_list[12], (D, FF), D ** -0.5, 0.15625, ((0, 8),))
    w_down = centred(key_list[13], (FF, D), FF ** -0.5, 0.09375, ((0, 8),))
    output_grad = centred(key_list[14], (SEQS, SLOTS, D), 1.0, 6.0, ((0, 8), (1, 4)))
    return dict(layer_input=layer_input, lengths=lengths, norm_attn=norm_attn, w_query=w_query, w_key=w_key, w_value=w_value, w_ogate=w_ogate, w_forget=w_forget, forget_bias=forget_bias, w_out=w_out, norm_ffn=norm_ffn, w_gate=w_gate, w_up=w_up, w_down=w_down, output_grad=output_grad)


@jax.custom_vjp
def low(v):
    return lax.optimization_barrier(v.astype(jnp.bfloat16)).astype(jnp.float32)

@jax.custom_vjp
def low_back(v):
    return v

def low_keep(v):
    return (low(v), None)

def low_pass(kept, grad):
    return (grad,)

def back_keep(v):
    return (v, None)

def back_low(kept, grad):
    return (low(grad),)
low.defvjp(low_keep, low_pass)
low_back.defvjp(back_keep, back_low)
EPS = 1e-06
NEG_FILL = -1e+30

def highest(left, right):
    return jnp.dot(left, right, precision=lax.Precision.HIGHEST)

def rms_norm(values, gain):
    return values * lax.rsqrt(lax.optimization_barrier(jnp.mean(values * values, axis=-1, keepdims=True)) + EPS) * gain

def attend(queries, keys_all, values_all, cumulative, length):
    slots, heads, head_size = queries.shape
    block = min(512, slots)
    scale = head_size ** (-0.5)
    columns = jnp.arange(slots, dtype=jnp.int32)

    def one_block(first):
        query_block = lax.dynamic_slice_in_dim(queries, first, block, 0)
        cum_rows = lax.dynamic_slice_in_dim(cumulative, first, block, 0)
        plain = jnp.einsum('qhd,khd->hqk', query_block, keys_all, precision=lax.Precision.HIGHEST) * scale
        plain = low_back(plain)
        plain = plain + cum_rows.T[:, :, None] - cumulative.T[:, None, :]
        rows = first + jnp.arange(block, dtype=jnp.int32)
        allowed = (columns[None, :] <= rows[:, None]) & (columns[None, :] < length)
        masked = jnp.where(allowed[None], plain, NEG_FILL)
        log_total = jax.nn.logsumexp(masked, axis=-1, keepdims=True)
        weights = low(jnp.exp(masked - log_total))
        return jnp.einsum('hqk,khd->qhd', weights, values_all, precision=lax.Precision.HIGHEST)
    firsts = jnp.arange(slots // block, dtype=jnp.int32) * block
    blocks = lax.map(jax.checkpoint(one_block), firsts)
    return blocks.reshape(slots, heads * head_size)

def forward(inputs, length, norm_attn, w_query, w_key, w_value, w_ogate, w_forget, forget_bias, w_out, norm_ffn, w_gate, w_up, w_down):
    slots = inputs.shape[0]
    heads = forget_bias.shape[0]
    head_size = w_query.shape[1] // heads
    normed_attn = low(rms_norm(inputs, norm_attn))
    queries = low_back(low(highest(normed_attn, w_query)))
    keys_all = low_back(low(highest(normed_attn, w_key)))
    values_all = low_back(low(highest(normed_attn, w_value)))
    gate_pre = low_back(highest(normed_attn, w_ogate))
    forget_pre = low_back(low(highest(normed_attn, w_forget)))
    cumulative = jnp.cumsum(jax.nn.log_sigmoid(forget_pre + forget_bias), axis=0)
    attended = attend(queries.reshape(slots, heads, head_size), keys_all.reshape(slots, heads, head_size), values_all.reshape(slots, heads, head_size), cumulative, length)
    attended = low_back(low(attended))
    gated = low(attended * jax.nn.sigmoid(gate_pre))
    middle = inputs + low_back(highest(gated, w_out))
    normed_ffn = low(rms_norm(middle, norm_ffn))
    gate = low_back(highest(normed_ffn, w_gate))
    upward = low_back(highest(normed_ffn, w_up))
    hidden = low(jax.nn.silu(gate) * upward)
    return middle + low_back(highest(hidden, w_down))

def reference(layer_input, lengths, norm_attn, w_query, w_key, w_value, w_ogate, w_forget, forget_bias, w_out, norm_ffn, w_gate, w_up, w_down, output_grad):
    params = tuple((p.astype(jnp.float32) for p in (norm_attn, w_query, w_key, w_value, w_ogate, w_forget, forget_bias, w_out, norm_ffn, w_gate, w_up, w_down)))

    def per_sequence(totals, item):
        inputs, length, cotangent = item
        valid_slots = (jnp.arange(inputs.shape[0], dtype=jnp.int32) < length).astype(jnp.float32)

        def run(values, *weights):
            return forward(values, length, *weights)
        result, pull = jax.vjp(run, inputs.astype(jnp.float32), *params)
        grads = pull(cotangent.astype(jnp.float32) * valid_slots[:, None])
        totals = tuple((total + grad for total, grad in zip(totals, grads[1:])))
        return (totals, (result.astype(jnp.bfloat16), grads[0]))
    start = tuple((jnp.zeros_like(p) for p in params))
    totals, (outputs, grad_inputs) = lax.scan(per_sequence, start, (layer_input, lengths, output_grad))
    return (outputs, grad_inputs, totals[0], totals[1], totals[2], totals[3], totals[4], totals[5], totals[6], totals[7], totals[8], totals[9], totals[10], totals[11])
```

```python
import jax
import jax.numpy as jnp
from jax import lax
from jax.sharding import PartitionSpec as P

EPS = 1e-06
NEG_FILL = -1e30
BF16 = jnp.bfloat16
F32 = jnp.float32


def product(left, right):
    return jnp.dot(left, right, preferred_element_type=F32)


def product_tn(left, right):
    return lax.dot_general(left, right, (((0,), (0,)), ((), ())), preferred_element_type=F32)


def product_nt(left, right):
    return lax.dot_general(left, right, (((1,), (1,)), ((), ())), preferred_element_type=F32)


def rms_norm(values, gain):
    return values * lax.rsqrt(jnp.mean(values * values, axis=-1, keepdims=True) + EPS) * gain


def gate_product(attended, gate_pre):
    return attended * jax.nn.sigmoid(gate_pre)


def swiglu(gate, upward):
    return jax.nn.silu(gate) * upward


def gather_rows(shard):
    return lax.all_gather(shard, "wshard", axis=0, tiled=True)


def scatter_rows(partial):
    return lax.psum_scatter(partial.astype(BF16), "wshard", scatter_dimension=0, tiled=True)


def gather_slots(shard):
    return lax.all_gather(shard, "seq", axis=0, tiled=True)


def scatter_slots(partial):
    return lax.psum_scatter(
        partial.astype(BF16), "seq", scatter_dimension=0, tiled=True
    ).astype(F32)


def share_columns(share):
    return lax.all_gather(share, "seq", axis=1, tiled=True).astype(F32)


def block_scores(query_block, key_block, cum_rows, cum_keys, first_row, length, scale):
    plain = (
        jnp.einsum("qhd,khd->hqk", query_block, key_block, preferred_element_type=F32) * scale
    )
    plain = plain + cum_rows.T[:, :, None] - cum_keys.T[:, None, :]
    rows = first_row + jnp.arange(query_block.shape[0], dtype=jnp.int32)
    columns = jnp.arange(key_block.shape[0], dtype=jnp.int32)
    allowed = (columns[None, :] <= rows[:, None]) & (columns[None, :] < length)
    return jnp.where(allowed[None], plain, NEG_FILL)


def attention_forward(query, key, value, cumulative, length, scale, block):
    slots = query.shape[0]
    blocks = []
    log_totals = []
    for first in range(0, slots, block):
        last = first + block
        masked = block_scores(
            query[first:last], key[:last], cumulative[first:last], cumulative[:last],
            first, length, scale,
        )
        log_total = jax.nn.logsumexp(masked, axis=-1, keepdims=True)
        probability = jnp.exp(masked - log_total).astype(BF16)
        blocks.append(
            jnp.einsum("hqk,khd->qhd", probability, value[:last], preferred_element_type=F32)
        )
        log_totals.append(log_total)
    return jnp.concatenate(blocks, axis=0).astype(BF16), log_totals


def attention_backward(query, key, value, grad, cumulative, log_totals, length, scale, block):
    slots, heads, size = query.shape
    grad_query = []
    grad_key = jnp.zeros((slots, heads, size), F32)
    grad_value = jnp.zeros((slots, heads, size), F32)
    grad_cum = jnp.zeros((slots, heads), F32)
    for number, first in enumerate(range(0, slots, block)):
        last = first + block
        masked = block_scores(
            query[first:last], key[:last], cumulative[first:last], cumulative[:last],
            first, length, scale,
        )
        probability = jnp.exp(masked - log_totals[number])
        probability_low = probability.astype(BF16)
        grad_block = grad[first:last]
        grad_probability = jnp.einsum(
            "qhd,khd->hqk", grad_block, value[:last], preferred_element_type=F32
        )
        row_dot = jnp.sum(grad_probability * probability, axis=-1, keepdims=True)
        score_terms = probability * (grad_probability - row_dot)
        grad_scores = score_terms.astype(BF16)
        grad_cum = grad_cum.at[first:last].add(jnp.sum(score_terms, axis=2).T)
        grad_cum = grad_cum.at[:last].add(-jnp.sum(score_terms, axis=1).T)
        grad_query.append(
            jnp.einsum("hqk,khd->qhd", grad_scores, key[:last], preferred_element_type=F32)
        )
        grad_key = grad_key.at[:last].add(
            jnp.einsum("hqk,qhd->khd", grad_scores, query[first:last], preferred_element_type=F32)
        )
        grad_value = grad_value.at[:last].add(
            jnp.einsum("hqk,qhd->khd", probability_low, grad_block, preferred_element_type=F32)
        )
    grad_query = (jnp.concatenate(grad_query, axis=0) * scale).astype(BF16)
    return grad_query, (grad_key * scale).astype(BF16), grad_value.astype(BF16), grad_cum


def on_device(
    layer_input, lengths, norm_attn, w_query, w_key, w_value, w_ogate, w_forget, forget_bias,
    w_out, norm_ffn, w_gate, w_up, w_down, output_grad,
):
    tokens, width = layer_input.shape[1:]
    heads = forget_bias.shape[0]
    groups = lax.axis_size("seq")
    owners = lax.axis_size("wshard")
    local_heads = heads // groups
    head_size = width // heads
    slots = tokens * groups
    part = width // groups
    units = w_gate.shape[1]
    own_units = units // owners
    piece = own_units // groups
    local_units = units // groups
    block = min(512, slots)
    scale = head_size ** (-0.5)
    length = lengths[0]
    rank = lax.axis_index("seq")
    positions = rank * tokens + jnp.arange(tokens, dtype=jnp.int32)
    valid_slots = (positions < length).astype(F32)[:, None]
    inputs = layer_input[0].astype(F32)
    cotangent = output_grad[0].astype(F32) * valid_slots

    def columns(weight):
        return lax.dynamic_slice_in_dim(weight, rank * part, part, 1)

    def unit_columns(weight):
        cut = lax.dynamic_index_in_dim(
            weight.reshape(-1, owners, groups, piece), rank, 2, keepdims=False
        )
        return cut.reshape(-1, local_units)

    pad = (-local_heads) % 128
    forget_columns = jnp.pad(
        lax.dynamic_slice_in_dim(w_forget, rank * local_heads, local_heads, 1), ((0, 0), (0, pad))
    )
    normed_attn = gather_slots(rms_norm(inputs, norm_attn).astype(BF16))
    full_attn = gather_rows(
        jnp.concatenate(
            [columns(w_query), columns(w_key), columns(w_value), columns(w_ogate), forget_columns],
            axis=1,
        )
    )
    cut_out = gather_rows(columns(w_out))
    full_out = lax.all_to_all(cut_out, "seq", split_axis=0, concat_axis=1, tiled=True)
    full_gate_up = gather_rows(
        jnp.concatenate([unit_columns(w_gate), unit_columns(w_up)], axis=1)
    )
    full_down = gather_rows(lax.dynamic_slice_in_dim(w_down, rank * piece, piece, 0))
    cotangent_low = gather_slots(cotangent.astype(BF16))

    query = product(normed_attn, full_attn[:, :part]).astype(BF16)
    key = product(normed_attn, full_attn[:, part : 2 * part]).astype(BF16)
    value = product(normed_attn, full_attn[:, 2 * part : 3 * part]).astype(BF16)
    gate_pre = product(normed_attn, full_attn[:, 3 * part : 4 * part])
    forget_pre = product(normed_attn, full_attn[:, 4 * part :])[:, :local_heads].astype(BF16)
    query = query.reshape(slots, local_heads, head_size)
    key = key.reshape(slots, local_heads, head_size)
    value = value.reshape(slots, local_heads, head_size)
    bias_local = lax.dynamic_slice_in_dim(forget_bias, rank * local_heads, local_heads)
    forget_total = forget_pre.astype(F32) + bias_local
    log_forget, pull_forget = jax.vjp(jax.nn.log_sigmoid, forget_total)
    cumulative = jnp.cumsum(log_forget, axis=0)
    head_output, log_totals = attention_forward(
        query, key, value, cumulative, length, scale, block
    )
    attended = head_output.reshape(slots, part).astype(F32)
    gated_full, pull_gate = jax.vjp(gate_product, attended, gate_pre)
    gated = gated_full.astype(BF16)
    middle = inputs + scatter_slots(product(gated, full_out))

    normed_ffn_full, pull_ffn_norm = jax.vjp(rms_norm, middle, norm_ffn)
    normed_ffn = gather_slots(normed_ffn_full.astype(BF16))
    gate_value = product(normed_ffn, full_gate_up[:, :local_units])
    up_value = product(normed_ffn, full_gate_up[:, local_units:])
    hidden_full, pull_swiglu = jax.vjp(swiglu, gate_value, up_value)
    hidden = hidden_full.astype(BF16)
    result = middle + scatter_slots(product(hidden, full_down))
    layer_output = result.astype(BF16)[None]

    grad_hidden = product_nt(cotangent_low, full_down)
    grad_gate_full, grad_up_full = pull_swiglu(grad_hidden)
    grad_gate_up = jnp.concatenate(
        [grad_gate_full.astype(BF16), grad_up_full.astype(BF16)], axis=1
    )
    grad_normed_ffn = scatter_slots(product_nt(grad_gate_up, full_gate_up))
    share_down = scatter_rows(product_tn(hidden, cotangent_low))
    share_gate_up = scatter_rows(product_tn(normed_ffn, grad_gate_up))
    grad_middle_part, grad_norm_ffn = pull_ffn_norm(grad_normed_ffn)
    grad_middle = cotangent + grad_middle_part
    grad_branch = gather_slots(grad_middle.astype(BF16))
    grad_gated = product_nt(grad_branch, full_out)
    grad_w_out = product_tn(gated, grad_branch).astype(BF16)
    share_out = scatter_rows(
        lax.all_to_all(grad_w_out, "seq", split_axis=1, concat_axis=0, tiled=True)
    )
    grad_attended_full, grad_gate_pre_full = pull_gate(grad_gated)
    grad_attended = grad_attended_full.astype(BF16).reshape(slots, local_heads, head_size)
    grad_gate_pre = grad_gate_pre_full.astype(BF16)
    grad_query, grad_key, grad_value, grad_cum = attention_backward(
        query, key, value, grad_attended, cumulative, log_totals, length, scale, block
    )
    grad_log_forget = jnp.flip(jnp.cumsum(jnp.flip(grad_cum, 0), axis=0), 0)
    grad_forget_total = pull_forget(grad_log_forget)[0]
    grad_bias_local = jnp.sum(grad_forget_total, axis=0)
    grad_bias = lax.dynamic_update_slice_in_dim(
        jnp.zeros((heads,), F32), grad_bias_local, rank * local_heads, 0
    )
    grad_attn = jnp.concatenate(
        [
            grad_query.reshape(slots, part),
            grad_key.reshape(slots, part),
            grad_value.reshape(slots, part),
            grad_gate_pre,
            jnp.pad(grad_forget_total.astype(BF16), ((0, 0), (0, pad))),
        ],
        axis=1,
    )
    grad_normed_attn = scatter_slots(product_nt(grad_attn, full_attn))
    share_attn = scatter_rows(product_tn(normed_attn, grad_attn))
    unused_normed, pull_attn_norm = jax.vjp(rms_norm, inputs, norm_attn)
    grad_input_part, grad_norm_attn = pull_attn_norm(grad_normed_attn)
    grad_input = (grad_middle + grad_input_part)[None]

    rows = w_query.shape[0]
    all_down = lax.all_gather(share_down, "seq", axis=0, tiled=True).astype(F32)
    all_gate_up = lax.all_gather(share_gate_up, "seq", axis=0, tiled=False)
    all_gate_up = all_gate_up.reshape(groups, rows, 2, owners, piece).transpose(2, 1, 3, 0, 4)
    all_gate_up = all_gate_up.reshape(2, rows, units).astype(F32)
    all_out = share_columns(share_out)
    all_attn = lax.all_gather(share_attn, "seq", axis=0, tiled=False)

    def whole(first, size):
        cut = all_attn[:, :, first : first + size].transpose(1, 0, 2)
        return cut.reshape(rows, groups * size).astype(F32)

    small = lax.psum((grad_norm_attn, grad_norm_ffn, grad_bias), ("seq", "wshard"))
    return (
        layer_output,
        grad_input,
        small[0],
        whole(0, part),
        whole(part, part),
        whole(2 * part, part),
        whole(3 * part, part),
        whole(4 * part, local_heads),
        small[2],
        all_out,
        small[1],
        all_gate_up[0],
        all_gate_up[1],
        all_down,
    )


def solution(mesh):
    rows = P("wshard", None)
    slots = P("wshard", "seq", None)
    return jax.shard_map(
        on_device,
        mesh=mesh,
        in_specs=(
            slots, P("wshard"), P(), rows, rows, rows, rows, rows, P(), rows, P(), rows, rows,
            rows, slots,
        ),
        out_specs=(
            slots, slots, P(), rows, rows, rows, rows, rows, P(), rows, P(), rows, rows, rows,
        ),
        check_vma=False,
    )
```
